32 devices in a mesh: sub: 16 (over z, y, core), col: 2 (over x).
Axes of the slice: x: 2, y: 2, z: 4, core: 2. Of those that a mesh axis runs over, the one named last changes fastest.
Arguments:
- interior_inverse: bfloat16 [16, 3072, 3072], P('sub', 'col'), may hold values from -1 to 2
- interface_coupling: bfloat16 [16, 3072, 512], P('sub', 'col'), may hold values from -0.109375 to 0.109375
- boundary_stiffness: float32 [16, 512, 512], P('sub', 'col'), may hold values from -3 to 3
- interior_mass: float32 [16, 3072], P('sub', 'col'), may hold values from 0.2 to 2
- boundary_mass: float32 [16, 512], P('sub', 'col'), may hold values from 0.2 to 2
- interior_modes: bfloat16 [16, 200, 3072], P('sub', None, 'col'), may hold values from -0.3125 to 0.3125
- block_map: int32 [16, 4], P('sub'), may hold values from 0 to 31, as said below
- trial_vectors: bfloat16 [64, 2, 2048], P(None, None, 'sub'), may hold values from -6 to 6
Outputs:
- reduced_stiffness: bfloat16 [2, 2048, 16, 256], P(None, 'sub', None, 'col')
- reduced_mass: bfloat16 [2, 2048, 16, 256], P(None, 'sub', None, 'col')
- modal_coupling: float32 [16, 64, 200], P('sub')
The draws below stay inside these ranges and needn't reach their ends.
Inputs may be any that keep to these rules, and one draw needn't show every extreme that they name: `block_map`: row s lists the four blocks (s - 1) mod 16, s, ((s - 1) mod 16) + 16 and s + 16 in some order.
All inputs are finite; a program needn't handle non-finite values.
Results may differ from the reference program's by a relative error of at most 0.008.
Values may be sent and summed in bfloat16 or wider, within the bound.
No kernel may reach another device: no remote copies, remote signals or barrier semaphores. Data moves between devices by JAX's collectives and lax.ppermute only.
A program may use at most 64 MiB of HBM per device.

```python
import math
import jax
import jax.numpy as jnp
from jax import lax

NI = 3072
NB = 512
BLK = 128
MODES = 200
TRIAL = 64
NSUB = 16
CC = 16
N_COL = 2


def draw_interior_inverse(key, part):

    def single(sub_key):
        first_key, second_key = jax.random.split(sub_key)
        spread_part = jax.random.truncated_normal(first_key, -4.0, 4.0, (NI, NI), jnp.float32) * (0.5 / math.sqrt(NI))
        diagonal_values = jax.random.uniform(second_key, (NI,), jnp.float32, 0.5, 1.5)
        on_diagonal = jnp.arange(NI, dtype=jnp.int32)[:, None] == jnp.arange(NI, dtype=jnp.int32)[None, :]
        return (spread_part + jnp.where(on_diagonal, diagonal_values[:, None], 0.0)).astype(jnp.bfloat16)
    return lax.map(single, jax.random.split(key, NSUB))


def draw_block_map(key, part):
    scores = jax.random.randint(key, (NSUB, 4), 0, 1 << 20, dtype=jnp.int32) * 4 + jnp.arange(4, dtype=jnp.int32)[None, :]
    ordering = jnp.argsort(scores, axis=1, stable=True).astype(jnp.int32)
    sub_ids = jnp.arange(NSUB, dtype=jnp.int32)[:, None]
    previous_ids = (sub_ids + NSUB - 1) % NSUB
    table = jnp.concatenate([previous_ids, sub_ids, previous_ids + NSUB, sub_ids + NSUB], axis=1)
    return jnp.take_along_axis(table, ordering, axis=1)


def steps_of(rng, dims, shards, smallest, largest):
    def one(position, blocks):
        steps = jax.random.uniform(jax.random.fold_in(jax.random.fold_in(rng, 6), position), (blocks,), jnp.float32, smallest / len(shards), largest / len(shards))
        return jnp.repeat(jnp.exp(steps), dims[position] // blocks).reshape((-1,) + (1,) * (len(dims) - position - 1))

    factor_of = one(*shards[0])
    for cut in shards[1:]:
        factor_of = factor_of * one(*cut)
    return factor_of


def bell_draw(key, shape, spread, most, pieces=(), kind=jnp.bfloat16):
    factor_of = steps_of(key, shape, pieces, -0.22, 0.18) if pieces else 1.0
    array = jax.random.normal(key, shape, jnp.float32) * spread * factor_of
    return jnp.minimum(jnp.maximum(array, -most), most).astype(kind)


def setup_inputs(seed: int = 0) -> dict:
    keys = jax.random.split(jax.random.key(seed), 9)
    return {
        "interior_inverse": draw_interior_inverse(jax.random.fold_in(keys[8], 71), 0),
        "interface_coupling": bell_draw(keys[1], (NSUB, NI, NB), NI ** -0.5, 0.109375, ((0, 16), (1, 2))),
        "boundary_stiffness": bell_draw(keys[2], (NSUB, NB, NB), 0.5, 3.0, ((0, 16), (1, 2)), jnp.float32),
        "interior_mass": jnp.clip(jnp.exp(math.log(2.0) - 2.3025851 * jax.random.uniform(keys[3], (NSUB, NI), jnp.float32) ** steps_of(keys[3], (NSUB, NI), ((0, 16), (1, 2)), -0.2, 0.2)), 0.2, 2.0),
        "boundary_mass": jnp.clip(jnp.exp(math.log(2.0) - 2.3025851 * jax.random.uniform(keys[4], (NSUB, NB), jnp.float32) ** steps_of(keys[4], (NSUB, NB), ((0, 16), (1, 2)), -0.2, 0.2)), 0.2, 2.0),
        "interior_modes": bell_draw(keys[5], (NSUB, MODES, NI), (NI // 8) ** -0.5, 0.3125, ((0, 16), (2, 2))),
        "block_map": draw_block_map(jax.random.fold_in(keys[8], 71), 0),
        "trial_vectors": bell_draw(keys[7], (TRIAL, 2, NSUB * BLK), 1.0, 6.0, ((2, 16),)),
    }


def condense(operands):
    inverse_block, coupling_block, stiffness_block, mass_interior, mass_boundary, modes_block = operands
    guyan = (-jnp.dot(inverse_block, coupling_block, preferred_element_type=jnp.float32)).astype(jnp.bfloat16)
    condensed_stiffness = stiffness_block + jnp.dot(coupling_block.T, guyan, preferred_element_type=jnp.float32)
    weighted = (mass_interior[:, None] * guyan.astype(jnp.float32)).astype(jnp.bfloat16)
    condensed_mass = jnp.diag(mass_boundary) + jnp.dot(guyan.T, weighted, preferred_element_type=jnp.float32)
    coupling_matrix = jnp.dot(modes_block, weighted, preferred_element_type=jnp.float32)
    return condensed_stiffness, condensed_mass, coupling_matrix


def reference(interior_inverse, interface_coupling, boundary_stiffness, interior_mass, boundary_mass, interior_modes, block_map, trial_vectors):
    stiff_all, mass_all, couple_all = lax.map(condense, (interior_inverse, interface_coupling, boundary_stiffness, interior_mass, boundary_mass, interior_modes))
    blocks_total = 2 * NSUB
    trial_blocks = trial_vectors.reshape(TRIAL, blocks_total, BLK)

    def couple(operands):
        map_row, coupling_matrix = operands
        chosen = jnp.take(trial_blocks, map_row, axis=1).reshape(TRIAL, NB).astype(jnp.float32)
        return jnp.dot(chosen, coupling_matrix.T, precision=lax.Precision.HIGHEST)

    modal_coupling = lax.map(couple, (block_map, couple_all))
    cycles = jnp.arange(2, dtype=jnp.int32)
    global_blocks = jnp.arange(blocks_total, dtype=jnp.int32)

    def gather_panel(matrix, map_row, owner_row):
        rows_pick = (map_row[None, :] == cycles[:, None] * NSUB + owner_row).astype(jnp.float32)
        cols_pick = (map_row[:, None] == global_blocks[None, :]).astype(jnp.float32)
        shaped = matrix.reshape(NB // BLK, BLK, NB // BLK, BLK)
        return jnp.einsum('ri,ixjy,jc->rxcy', rows_pick, shaped, cols_pick, precision=lax.Precision.HIGHEST)

    def assemble(owner_row):
        next_sub = (owner_row + 1) % NSUB
        stiffness = gather_panel(stiff_all[owner_row], block_map[owner_row], owner_row) + gather_panel(stiff_all[next_sub], block_map[next_sub], owner_row)
        massive = gather_panel(mass_all[owner_row], block_map[owner_row], owner_row) + gather_panel(mass_all[next_sub], block_map[next_sub], owner_row)
        return (stiffness.astype(jnp.bfloat16).reshape(2, BLK, CC, N_COL * BLK),
                massive.astype(jnp.bfloat16).reshape(2, BLK, CC, N_COL * BLK))

    panels_stiff, panels_mass = lax.map(assemble, jnp.arange(NSUB, dtype=jnp.int32))
    reduced_stiffness = jnp.transpose(panels_stiff, (1, 0, 2, 3, 4)).reshape(2, NSUB * BLK, CC, N_COL * BLK)
    reduced_mass = jnp.transpose(panels_mass, (1, 0, 2, 3, 4)).reshape(2, NSUB * BLK, CC, N_COL * BLK)
    return (reduced_stiffness, reduced_mass, modal_coupling)
```

```python
import functools
import jax
import jax.numpy as jnp
from jax import lax
from jax.experimental import pallas as pl
from jax.experimental.pallas import tpu as pltpu
from jax.sharding import PartitionSpec as P


def shifted(block, axis, distance):
    devices = range(lax.axis_size(axis))
    route = [((i - distance) % len(devices), i) for i in devices]
    return lax.ppermute(block, axis, route)


def shards(
    interior_inverse,
    interface_coupling,
    boundary_stiffness,
    interior_mass,
    boundary_mass,
    interior_modes,
    block_map,
    trial_vectors,
):
    inverse_rows = interior_inverse[0]
    coupling_rows = interface_coupling[0]
    boundary_width = coupling_rows.shape[1]
    block_size = trial_vectors.shape[2]
    block_count = boundary_width // block_size
    sub_count = lax.axis_size("sub")
    grid_columns = lax.axis_size("col")
    sub_index = lax.axis_index("sub")
    column_index = lax.axis_index("col")
    previous_sub = (sub_index + sub_count - 1) % sub_count
    cycles = 2 * sub_count // grid_columns
    highest = lax.Precision.HIGHEST
    guyan_sum = jnp.dot(
        inverse_rows,
        lax.all_gather(coupling_rows, "col", axis=0, tiled=True),
        preferred_element_type=jnp.float32,
    )
    guyan = (-guyan_sum).astype(jnp.bfloat16)
    stiff_rows = boundary_stiffness[0]
    row_share = stiff_rows.shape[0]
    row_offset = column_index * row_share
    stiff_part = jnp.einsum("rb,rc->bc", coupling_rows, guyan, preferred_element_type=jnp.float32)
    stiff_part = lax.dynamic_update_slice_in_dim(
        stiff_part,
        lax.dynamic_slice_in_dim(stiff_part, row_offset, row_share, 0) + stiff_rows,
        row_offset,
        0,
    )
    weighted = (interior_mass[0][:, None] * guyan.astype(jnp.float32)).astype(jnp.bfloat16)
    mass_part = jnp.einsum("rb,rc->bc", guyan, weighted, preferred_element_type=jnp.float32)
    diagonal_rows = jnp.where(
        jnp.arange(boundary_width, dtype=jnp.int32)[None, :]
        == (row_offset + jnp.arange(row_share, dtype=jnp.int32))[:, None],
        boundary_mass[0][:, None],
        0.0,
    )
    mass_part = lax.dynamic_update_slice_in_dim(
        mass_part,
        lax.dynamic_slice_in_dim(mass_part, row_offset, row_share, 0) + diagonal_rows,
        row_offset,
        0,
    )
    previous_trial = shifted(trial_vectors, "sub", 1)
    candidates = jnp.concatenate([trial_vectors, previous_trial], axis=1)
    labels = jnp.stack([sub_index, sub_index + sub_count, previous_sub, previous_sub + sub_count])
    own_map = block_map[0]
    chooser = (own_map[:, None] == labels[None, :]).astype(jnp.bfloat16)
    local_trial = (
        jnp.einsum("tkb,ik->tib", candidates, chooser, preferred_element_type=jnp.float32)
        .astype(jnp.bfloat16)
        .reshape(trial_vectors.shape[0], boundary_width)
    )
    projected = jnp.einsum("rj,tj->tr", weighted, local_trial, preferred_element_type=jnp.float32)
    small_part = jnp.einsum(
        "tr,mr->tm", projected, interior_modes[0].astype(jnp.float32), precision=highest
    )
    stiffness, mass_sum, small_sum = lax.psum((stiff_part, mass_part, small_part), "col")
    stiff_blocks = stiffness.reshape(block_count, block_size, block_count, block_size)
    mass_blocks = mass_sum.reshape(block_count, block_size, block_count, block_size)
    row_cycles = jnp.arange(2, dtype=jnp.int32)

    def rows_for(owner_row):
        return (own_map[None, :] == row_cycles[:, None] * sub_count + owner_row).astype(jnp.float32)

    placement = (
        own_map[:, None]
        == jnp.arange(cycles, dtype=jnp.int32)[None, :] * grid_columns + column_index
    ).astype(jnp.float32)

    def select_rows(selection, blocks):
        return jnp.einsum("ri,ixjy->rxjy", selection, blocks, precision=highest)

    def spread(panel, where):
        return jnp.einsum("rxjy,jc->rxcy", panel, where, precision=highest)

    own_selection = rows_for(sub_index)
    own_stiff = spread(select_rows(own_selection, stiff_blocks), placement)
    own_mass = spread(select_rows(own_selection, mass_blocks), placement)
    leaving = rows_for(previous_sub)
    leaving_stiff = select_rows(leaving, stiff_blocks)
    leaving_mass = select_rows(leaving, mass_blocks)
    neighbour_stiff, neighbour_mass, neighbour_place = shifted(
        (leaving_stiff, leaving_mass, placement), "sub", -1
    )
    reduced_stiffness = (own_stiff + spread(neighbour_stiff, neighbour_place)).astype(jnp.bfloat16)
    reduced_mass = (own_mass + spread(neighbour_mass, neighbour_place)).astype(jnp.bfloat16)
    return (reduced_stiffness, reduced_mass, small_sum[None])


def class_table(own_map, sub_index, column_index, sub_count):
    cycle = own_map // sub_count
    parity = own_map % 2
    slots = jnp.arange(4, dtype=jnp.int32)
    wanted_parity = jnp.where(slots < 2, column_index, 1 - column_index)
    hit = (parity[None, :] == wanted_parity[:, None]) & (cycle[None, :] == (slots % 2)[:, None])
    places = jnp.sum(jnp.where(hit, slots[None, :], 0), axis=1)
    is_even = (sub_index % 2 == column_index).astype(jnp.int32)
    return jnp.concatenate([places, jnp.stack([column_index, is_even])]).astype(jnp.int32)


def pick_kernel(table_ref, source_ref, out_ref):
    out_ref[...] = source_ref[...]


def pick_columns(table, rows, offset, block):
    depth = rows.shape[0]
    return pl.pallas_call(
        pick_kernel,
        grid_spec=pltpu.PrefetchScalarGridSpec(
            num_scalar_prefetch=1,
            grid=(2,),
            in_specs=[pl.BlockSpec((depth, block), lambda p, t: (0, t[offset + p]))],
            out_specs=pl.BlockSpec((depth, block), lambda p, t: (0, p)),
        ),
        out_shape=jax.ShapeDtypeStruct((depth, 2 * block), rows.dtype),
        cost_estimate=cost(0, 4 * depth * block * 2),
    )(table, rows)


def cost(flops, moved):
    return pl.CostEstimate(flops=int(flops), bytes_accessed=int(moved), transcendentals=0)


def tdot(a, b):
    return lax.dot_general(a, b, (((0,), (0,)), ((), ())), preferred_element_type=jnp.float32)


def ndot(a, b):
    return jnp.dot(a, b, preferred_element_type=jnp.float32)


def rdot(a, b):
    return lax.dot_general(a, b, (((1,), (1,)), ((), ())), preferred_element_type=jnp.float32)


def edge_block(table_ref, edge_ref, row_slot, column_slot, block):
    local = table_ref[row_slot] - 2 * table_ref[4]
    inside = (local >= 0) & (local < 2)
    row = pl.multiple_of(jnp.clip(local, 0, 1) * block, block)
    column = pl.multiple_of(table_ref[column_slot] * block, block)
    return jnp.where(inside, edge_ref[pl.ds(row, block), pl.ds(column, block)], 0.0)


def edge_panel(table_ref, edge_ref, row_base, column_base, block):
    return jnp.concatenate(
        [
            jnp.concatenate(
                [
                    edge_block(table_ref, edge_ref, row_base + p, column_base + k, block)
                    for k in range(2)
                ],
                axis=1,
            )
            for p in range(2)
        ],
        axis=0,
    )


def edge_diagonal(table_ref, weight_ref, base, block):
    width = 2 * block
    rows = lax.broadcasted_iota(jnp.int32, (width, width), 0)
    columns = lax.broadcasted_iota(jnp.int32, (width, width), 1)
    parts = []
    for p in range(2):
        local = table_ref[base + p] - 2 * table_ref[4]
        inside = (local >= 0) & (local < 2)
        parts.append(jnp.where(inside, weight_ref[pl.ds(jnp.clip(local, 0, 1), 1), :], 0.0))
    return jnp.where(rows == columns, jnp.concatenate(parts, axis=1), 0.0)


def scaled(mass, g):
    half = mass.shape[1]
    wide = g.astype(jnp.float32)
    return jnp.concatenate([wide[:, :half] * mass, wide[:, half:] * mass], axis=1).astype(jnp.bfloat16)


def first_kernel(
    block,
    table_ref,
    near_ref,
    far_ref,
    mine_ref,
    theirs_ref,
    got_ref,
    mass_ref,
    edge_ref,
    weight_ref,
    g_ref,
    w_ref,
    pre_ref,
    low_ref,
    high_ref,
    square_ref,
    stiff_acc,
    mass_acc,
):
    step = pl.program_id(0)
    depth = near_ref.shape[0]
    near = near_ref[...]
    g = (-(ndot(near, theirs_ref[...]) + ndot(far_ref[...], got_ref[...]))).astype(jnp.bfloat16)
    w = scaled(mass_ref[...], g)
    g_ref[...] = g
    w_ref[...] = w
    pre_ref[...] = ndot(near, mine_ref[...])
    here = pl.ds(pl.multiple_of(step * depth, depth), depth)

    @pl.when(step == 0)
    def _():
        stiff_acc[...] = jnp.zeros_like(stiff_acc)
        mass_acc[...] = jnp.zeros_like(mass_acc)

    stiff_acc[0] += tdot(theirs_ref[here, :], g)
    stiff_acc[1] += tdot(mine_ref[here, :], g)
    mass_acc[...] += tdot(g, w)

    @pl.when(step == pl.num_programs(0) - 1)
    def _():
        even = table_ref[5] == 1
        of_theirs = (stiff_acc[0] + edge_panel(table_ref, edge_ref, 2, 2, block)).astype(jnp.bfloat16)
        of_mine = (stiff_acc[1] + edge_panel(table_ref, edge_ref, 0, 2, block)).astype(jnp.bfloat16)
        low_ref[...] = jnp.where(even, of_theirs, of_mine)
        high_ref[...] = jnp.where(even, of_mine, of_theirs)
        square_ref[...] = (mass_acc[...] + edge_diagonal(table_ref, weight_ref, 2, block)).astype(
            jnp.bfloat16
        )


def second_kernel(
    table_ref,
    far_ref,
    got_ref,
    pre_ref,
    other_w_ref,
    mass_ref,
    square_ref,
    modes_ref,
    trial_mine_ref,
    trial_theirs_ref,
    g_ref,
    w_ref,
    low_ref,
    high_ref,
    mass_acc,
    small_acc,
):
    step = pl.program_id(0)
    g = (-(pre_ref[...] + ndot(far_ref[...], got_ref[...]))).astype(jnp.bfloat16)
    w = scaled(mass_ref[...], g)
    g_ref[...] = g
    w_ref[...] = w
    other = other_w_ref[...]

    @pl.when(step == 0)
    def _():
        mass_acc[...] = jnp.zeros_like(mass_acc)
        small_acc[...] = jnp.zeros_like(small_acc)

    mass_acc[...] += tdot(g, other)
    projected = rdot(trial_mine_ref[...], w) + rdot(trial_theirs_ref[...], other)
    upper = projected.astype(jnp.bfloat16)
    lower = (projected - upper.astype(jnp.float32)).astype(jnp.bfloat16)
    modes = modes_ref[...]
    small_acc[...] += rdot(upper, modes) + rdot(lower, modes)

    @pl.when(step == pl.num_programs(0) - 1)
    def _():
        even = table_ref[5] == 1
        mixed = mass_acc[...].astype(jnp.bfloat16)
        square = square_ref[...]
        width = square.shape[0]
        low_ref[...] = jnp.where(even, square, mixed)
        high_ref[pl.ds(0, width), :] = jnp.where(even, mixed, square)
        small = small_acc[...]
        count, modes_count = small.shape
        high_ref[pl.ds(width, count), :] = jnp.concatenate(
            [small, jnp.zeros((count, width - modes_count), jnp.float32)], axis=1
        ).astype(jnp.bfloat16)


def third_kernel(
    block,
    table_ref,
    g_ref,
    w_ref,
    other_g_ref,
    mine_ref,
    theirs_ref,
    edge_ref,
    weight_ref,
    low_ref,
    high_ref,
    acc,
):
    step = pl.program_id(0)

    @pl.when(step == 0)
    def _():
        acc[...] = jnp.zeros_like(acc)

    g = g_ref[...]
    w = w_ref[...]
    acc[0] += tdot(theirs_ref[...], g)
    acc[1] += tdot(mine_ref[...], g)
    acc[2] += tdot(other_g_ref[...], w)
    acc[3] += tdot(g, w)

    @pl.when(step == pl.num_programs(0) - 1)
    def _():
        even = table_ref[5] == 1
        stiff_theirs = acc[0] + edge_panel(table_ref, edge_ref, 2, 0, block)
        stiff_mine = acc[1] + edge_panel(table_ref, edge_ref, 0, 0, block)
        mass_theirs = acc[2]
        mass_mine = acc[3] + edge_diagonal(table_ref, weight_ref, 0, block)
        low_ref[0] = jnp.where(even, stiff_theirs, stiff_mine).astype(jnp.bfloat16)
        low_ref[1] = jnp.where(even, mass_theirs, mass_mine).astype(jnp.bfloat16)
        high_ref[0] = jnp.where(even, stiff_mine, stiff_theirs)
        high_ref[1] = jnp.where(even, mass_mine, mass_theirs)


def place_kernel(block, spots_ref, own_ref, high_ref, low_ref, cross_ref, out_ref):
    kept = own_ref[0] + high_ref[...].astype(jnp.float32)
    moved = low_ref[0].astype(jnp.float32) + cross_ref[...].astype(jnp.float32)
    count, cycles = out_ref.shape[1], out_ref.shape[2]
    lanes = lax.broadcasted_iota(jnp.int32, (count, cycles, block), 1)
    total = jnp.zeros((count, cycles, block), jnp.float32)
    for k in range(2):
        part = slice(k * block, (k + 1) * block)
        total += jnp.where(lanes == spots_ref[k], kept[:, part][:, None, :], 0.0)
        total += jnp.where(lanes == spots_ref[2 + k], moved[:, part][:, None, :], 0.0)
    out_ref[0] = total.astype(out_ref.dtype)


def place(spots, own, high, low, cross, which, cycles, block):
    width = 2 * block
    rows = min(64, block)
    steps = block // rows
    flat = lambda p, x, t: (p * steps + x, 0)
    deep = lambda p, x, t: (which, p * steps + x, 0)
    return pl.pallas_call(
        functools.partial(place_kernel, block),
        grid_spec=pltpu.PrefetchScalarGridSpec(
            num_scalar_prefetch=1,
            grid=(2, steps),
            in_specs=[
                pl.BlockSpec((1, rows, width), deep),
                pl.BlockSpec((rows, width), flat),
                pl.BlockSpec((1, rows, width), deep),
                pl.BlockSpec((rows, width), flat),
            ],
            out_specs=pl.BlockSpec((1, rows, cycles, block), lambda p, x, t: (p, x, 0, 0)),
        ),
        out_shape=jax.ShapeDtypeStruct((2, block, cycles, block), jnp.bfloat16),
        cost_estimate=cost(2 * block * cycles * block * 8, 4 * block * cycles * block),
    )(spots, own, high, low, cross)


def pair_shards(
    interior_inverse,
    interface_coupling,
    boundary_stiffness,
    interior_mass,
    boundary_mass,
    interior_modes,
    block_map,
    trial_vectors,
):
    inverse_rows = interior_inverse[0]
    coupling_rows = interface_coupling[0]
    edge = boundary_stiffness[0]
    depth, _ = inverse_rows.shape
    block = trial_vectors.shape[2]
    width = 2 * block
    trials = trial_vectors.shape[0]
    modes = interior_modes[0]
    modes_count = modes.shape[0]
    sub_count = lax.axis_size("sub")
    sub_index = lax.axis_index("sub")
    column_index = lax.axis_index("col")
    cycles = 2 * sub_count // 2
    table = class_table(block_map[0], sub_index, column_index, sub_count)
    even = table[5] == 1
    swap = [(0, 1), (1, 0)]
    both = ("sub", "col")
    back = [(i, (i - 1) % sub_count) for i in range(sub_count)]
    cross = [
        (2 * i + c, 2 * ((i - 1) % sub_count) + 1 - c) for i in range(sub_count) for c in range(2)
    ]
    mine = pick_columns(table, coupling_rows, 0, block)
    got_theirs = lax.ppermute(mine, "col", swap)
    theirs = pick_columns(table, coupling_rows, 2, block)
    got_mine = lax.ppermute(theirs, "col", swap)
    previous_trial = shifted(trial_vectors, "sub", 1)
    trial_high = trial_vectors.reshape(trials, width)
    trial_low = previous_trial.reshape(trials, width)
    trial_mine = jnp.where(even, trial_high, trial_low)
    trial_theirs = jnp.where(even, trial_low, trial_high)
    mass_columns = jnp.broadcast_to(interior_mass[0][:, None], (depth, block))
    weights = boundary_mass[0].reshape(2, block)

    tile = depth // 3
    steps = 3
    row = lambda i, t: (i, 0)
    whole = lambda i, t: (0, 0)
    bf16, f32 = jnp.bfloat16, jnp.float32
    arbitrary = pltpu.CompilerParams(dimension_semantics=("arbitrary",))
    g_theirs, w_theirs, pre, stiff_low, stiff_high, square = pl.pallas_call(
        functools.partial(first_kernel, block),
        grid_spec=pltpu.PrefetchScalarGridSpec(
            num_scalar_prefetch=1,
            grid=(steps,),
            in_specs=[
                pl.BlockSpec((tile, depth), lambda i, t: (i, t[4])),
                pl.BlockSpec((tile, depth), lambda i, t: (i, 1 - t[4])),
                pl.BlockSpec((depth, width), whole),
                pl.BlockSpec((depth, width), whole),
                pl.BlockSpec((depth, width), whole),
                pl.BlockSpec((tile, block), row),
                pl.BlockSpec(edge.shape, whole),
                pl.BlockSpec(weights.shape, whole),
            ],
            out_specs=[
                pl.BlockSpec((tile, width), row),
                pl.BlockSpec((tile, width), row),
                pl.BlockSpec((tile, width), row),
                pl.BlockSpec((width, width), whole),
                pl.BlockSpec((width, width), whole),
                pl.BlockSpec((width, width), whole),
            ],
            scratch_shapes=[pltpu.VMEM((2, width, width), f32), pltpu.VMEM((width, width), f32)],
        ),
        out_shape=[
            jax.ShapeDtypeStruct((depth, width), bf16),
            jax.ShapeDtypeStruct((depth, width), bf16),
            jax.ShapeDtypeStruct((depth, width), f32),
            jax.ShapeDtypeStruct((width, width), bf16),
            jax.ShapeDtypeStruct((width, width), bf16),
            jax.ShapeDtypeStruct((width, width), bf16),
        ],
        compiler_params=arbitrary,
        cost_estimate=cost(6 * depth * depth * width, 4 * depth * depth),
        name="first",
    )(table, inverse_rows, inverse_rows, mine, theirs, got_theirs, mass_columns, edge, weights)
    cross_stiff = lax.ppermute(stiff_low, both, cross)
    high_stiff = lax.ppermute(stiff_high, "col", swap)

    g_mine, w_mine, mass_low, mass_high = pl.pallas_call(
        second_kernel,
        grid_spec=pltpu.PrefetchScalarGridSpec(
            num_scalar_prefetch=1,
            grid=(steps,),
            in_specs=[
                pl.BlockSpec((tile, depth), lambda i, t: (i, 1 - t[4])),
                pl.BlockSpec((depth, width), whole),
                pl.BlockSpec((tile, width), row),
                pl.BlockSpec((tile, width), row),
                pl.BlockSpec((tile, block), row),
                pl.BlockSpec((width, width), whole),
                pl.BlockSpec((modes_count, tile), lambda i, t: (0, i)),
                pl.BlockSpec((trials, width), whole),
                pl.BlockSpec((trials, width), whole),
            ],
            out_specs=[
                pl.BlockSpec((tile, width), row),
                pl.BlockSpec((tile, width), row),
                pl.BlockSpec((width, width), whole),
                pl.BlockSpec((width + trials, width), whole),
            ],
            scratch_shapes=[
                pltpu.VMEM((width, width), f32),
                pltpu.VMEM((trials, modes_count), f32),
            ],
        ),
        out_shape=[
            jax.ShapeDtypeStruct((depth, width), bf16),
            jax.ShapeDtypeStruct((depth, width), bf16),
            jax.ShapeDtypeStruct((width, width), bf16),
            jax.ShapeDtypeStruct((width + trials, width), bf16),
        ],
        compiler_params=arbitrary,
        cost_estimate=cost(2 * depth * depth * width, 2 * depth * depth),
        name="second",
    )(
        table,
        inverse_rows,
        got_mine,
        pre,
        w_theirs,
        mass_columns,
        square,
        modes,
        trial_mine,
        trial_theirs,
    )
    high_mass = lax.ppermute(mass_high, "col", swap)
    cross_mass = lax.ppermute(mass_low, both, cross)

    low, own = pl.pallas_call(
        functools.partial(third_kernel, block),
        grid_spec=pltpu.PrefetchScalarGridSpec(
            num_scalar_prefetch=1,
            grid=(steps,),
            in_specs=[
                pl.BlockSpec((tile, width), row),
                pl.BlockSpec((tile, width), row),
                pl.BlockSpec((tile, width), row),
                pl.BlockSpec((tile, width), row),
                pl.BlockSpec((tile, width), row),
                pl.BlockSpec(edge.shape, whole),
                pl.BlockSpec(weights.shape, whole),
            ],
            out_specs=[
                pl.BlockSpec((2, width, width), lambda i, t: (0, 0, 0)),
                pl.BlockSpec((2, width, width), lambda i, t: (0, 0, 0)),
            ],
            scratch_shapes=[pltpu.VMEM((4, width, width), f32)],
        ),
        out_shape=[
            jax.ShapeDtypeStruct((2, width, width), bf16),
            jax.ShapeDtypeStruct((2, width, width), f32),
        ],
        compiler_params=arbitrary,
        cost_estimate=cost(8 * depth * width * width, 10 * depth * width),
        name="third",
    )(table, g_mine, w_mine, g_theirs, mine, theirs, edge, weights)
    low_here = lax.ppermute(low, "sub", back)

    high_base = jnp.where(even, sub_index, (sub_index + sub_count - 1) % sub_count)
    low_base = jnp.where(even, sub_index, (sub_index + 1) % sub_count)
    bases = jnp.stack([high_base, high_base + sub_count, low_base, low_base + sub_count])
    spots = (bases // 2).astype(jnp.int32)
    reduced_stiffness = place(spots, own, high_stiff, low_here, cross_stiff, 0, cycles, block)
    reduced_mass = place(spots, own, high_mass, low_here, cross_mass, 1, cycles, block)
    small = mass_high[width:, :modes_count].astype(f32) + high_mass[width:, :modes_count].astype(f32)
    return (reduced_stiffness, reduced_mass, small[None])


def solution(mesh):
    placed = (
        P("sub", "col", None),
        P("sub", "col", None),
        P("sub", "col", None),
        P("sub", "col"),
        P("sub", "col"),
        P("sub", None, "col"),
        P("sub", None),
        P(None, None, "sub"),
    )
    paired = mesh.shape["col"] == 2 and mesh.shape["sub"] % 2 == 0
    return jax.shard_map(
        pair_shards if paired else shards,
        mesh=mesh,
        in_specs=placed,
        out_specs=(P(None, "sub", None, "col"), P(None, "sub", None, "col"), P("sub", None, None)),
        check_vma=False,
    )
```

```python
import functools
import jax
import jax.numpy as jnp
from jax import lax
from jax.experimental import pallas as pl
from jax.experimental.pallas import tpu as pltpu
from jax.sharding import PartitionSpec as P


def shifted(block, axis, distance):
    devices = range(lax.axis_size(axis))
    route = [((i - distance) % len(devices), i) for i in devices]
    return lax.ppermute(block, axis, route)


def shards(
    interior_inverse,
    interface_coupling,
    boundary_stiffness,
    interior_mass,
    boundary_mass,
    interior_modes,
    block_map,
    trial_vectors,
):
    inverse_rows = interior_inverse[0]
    coupling_rows = interface_coupling[0]
    boundary_width = coupling_rows.shape[1]
    block_size = trial_vectors.shape[2]
    block_count = boundary_width // block_size
    sub_count = lax.axis_size("sub")
    grid_columns = lax.axis_size("col")
    sub_index = lax.axis_index("sub")
    column_index = lax.axis_index("col")
    previous_sub = (sub_index + sub_count - 1) % sub_count
    cycles = 2 * sub_count // grid_columns
    highest = lax.Precision.HIGHEST
    guyan_sum = jnp.dot(
        inverse_rows,
        lax.all_gather(coupling_rows, "col", axis=0, tiled=True),
        preferred_element_type=jnp.float32,
    )
    guyan = (-guyan_sum).astype(jnp.bfloat16)
    stiff_rows = boundary_stiffness[0]
    row_share = stiff_rows.shape[0]
    row_offset = column_index * row_share
    stiff_part = jnp.einsum("rb,rc->bc", coupling_rows, guyan, preferred_element_type=jnp.float32)
    stiff_part = lax.dynamic_update_slice_in_dim(
        stiff_part,
        lax.dynamic_slice_in_dim(stiff_part, row_offset, row_share, 0) + stiff_rows,
        row_offset,
        0,
    )
    weighted = (interior_mass[0][:, None] * guyan.astype(jnp.float32)).astype(jnp.bfloat16)
    mass_part = jnp.einsum("rb,rc->bc", guyan, weighted, preferred_element_type=jnp.float32)
    diagonal_rows = jnp.where(
        jnp.arange(boundary_width, dtype=jnp.int32)[None, :]
        == (row_offset + jnp.arange(row_share, dtype=jnp.int32))[:, None],
        boundary_mass[0][:, None],
        0.0,
    )
    mass_part = lax.dynamic_update_slice_in_dim(
        mass_part,
        lax.dynamic_slice_in_dim(mass_part, row_offset, row_share, 0) + diagonal_rows,
        row_offset,
        0,
    )
    previous_trial = shifted(trial_vectors, "sub", 1)
    candidates = jnp.concatenate([trial_vectors, previous_trial], axis=1)
    labels = jnp.stack([sub_index, sub_index + sub_count, previous_sub, previous_sub + sub_count])
    own_map = block_map[0]
    chooser = (own_map[:, None] == labels[None, :]).astype(jnp.bfloat16)
    local_trial = (
        jnp.einsum("tkb,ik->tib", candidates, chooser, preferred_element_type=jnp.float32)
        .astype(jnp.bfloat16)
        .reshape(trial_vectors.shape[0], boundary_width)
    )
    projected = jnp.einsum("rj,tj->tr", weighted, local_trial, preferred_element_type=jnp.float32)
    small_part = jnp.einsum(
        "tr,mr->tm", projected, interior_modes[0].astype(jnp.float32), precision=highest
    )
    stiffness, mass_sum, small_sum = lax.psum((stiff_part, mass_part, small_part), "col")
    stiff_blocks = stiffness.reshape(block_count, block_size, block_count, block_size)
    mass_blocks = mass_sum.reshape(block_count, block_size, block_count, block_size)
    row_cycles = jnp.arange(2, dtype=jnp.int32)

    def rows_for(owner_row):
        return (own_map[None, :] == row_cycles[:, None] * sub_count + owner_row).astype(jnp.float32)

    placement = (
        own_map[:, None]
        == jnp.arange(cycles, dtype=jnp.int32)[None, :] * grid_columns + column_index
    ).astype(jnp.float32)

    def select_rows(selection, blocks):
        return jnp.einsum("ri,ixjy->rxjy", selection, blocks, precision=highest)

    def spread(panel, where):
        return jnp.einsum("rxjy,jc->rxcy", panel, where, precision=highest)

    own_selection = rows_for(sub_index)
    own_stiff = spread(select_rows(own_selection, stiff_blocks), placement)
    own_mass = spread(select_rows(own_selection, mass_blocks), placement)
    leaving = rows_for(previous_sub)
    leaving_stiff = select_rows(leaving, stiff_blocks)
    leaving_mass = select_rows(leaving, mass_blocks)
    neighbour_stiff, neighbour_mass, neighbour_place = shifted(
        (leaving_stiff, leaving_mass, placement), "sub", -1
    )
    reduced_stiffness = (own_stiff + spread(neighbour_stiff, neighbour_place)).astype(jnp.bfloat16)
    reduced_mass = (own_mass + spread(neighbour_mass, neighbour_place)).astype(jnp.bfloat16)
    return (reduced_stiffness, reduced_mass, small_sum[None])


BF16, F32 = jnp.bfloat16, jnp.float32


def in_vmem(x):
    return pltpu.with_memory_space_constraint(x, pltpu.VMEM)


def cost(flops, moved):
    return pl.CostEstimate(flops=int(flops), bytes_accessed=int(moved), transcendentals=0)


def tdot(a, b):
    return lax.dot_general(a, b, (((0,), (0,)), ((), ())), preferred_element_type=F32)


def ndot(a, b):
    return jnp.dot(a, b, preferred_element_type=F32)


def rdot(a, b):
    return lax.dot_general(a, b, (((1,), (1,)), ((), ())), preferred_element_type=F32)


def is_even():
    return lax.rem(lax.axis_index("sub"), 2) == lax.axis_index("col")


def spot(map_ref, parity, cycle, sub_count):
    found = jnp.int32(0)
    for i in range(4):
        label = map_ref[0, i]
        hit = (lax.rem(label, 2) == parity) & (lax.div(label, sub_count) == cycle)
        found += jnp.where(hit, i, 0)
    return found


def spots(map_ref, sub_count):
    column = lax.axis_index("col")
    return [
        [spot(map_ref, parity, cycle, sub_count) for cycle in range(2)]
        for parity in (column, 1 - column)
    ]


def edge_panel(row_places, column_places, edge_ref, block):
    column = lax.axis_index("col")
    rows = []
    for place in row_places:
        local = place - 2 * column
        inside = (local >= 0) & (local < 2)
        row = pl.multiple_of(jnp.clip(local, 0, 1) * block, block)
        cells = []
        for other in column_places:
            start = pl.multiple_of(other * block, block)
            cells.append(jnp.where(inside, edge_ref[pl.ds(row, block), pl.ds(start, block)], 0.0))
        rows.append(jnp.concatenate(cells, axis=1))
    return jnp.concatenate(rows, axis=0)


def edge_diagonal(places, weight_ref, block):
    column = lax.axis_index("col")
    width = 2 * block
    rows = lax.broadcasted_iota(jnp.int32, (width, width), 0)
    columns = lax.broadcasted_iota(jnp.int32, (width, width), 1)
    parts = []
    for place in places:
        local = place - 2 * column
        inside = (local >= 0) & (local < 2)
        parts.append(jnp.where(inside, weight_ref[pl.ds(jnp.clip(local, 0, 1), 1), :], 0.0))
    return jnp.where(rows == columns, jnp.concatenate(parts, axis=1), 0.0)


def scaled(mass, g):
    half = mass.shape[1]
    wide = g.astype(F32)
    return jnp.concatenate([wide[:, :half] * mass, wide[:, half:] * mass], axis=1).astype(BF16)


def halves(array):
    upper = array.astype(BF16)
    return upper, (array - upper.astype(F32)).astype(BF16)


def pick_kernel(sub_count, block, map_ref, source_ref, mine_ref, head_ref, tail_ref, table_ref, stage_ref, sems):
    depth = source_ref.shape[0]
    head = head_ref.shape[0]
    pieces = 2
    rows = depth // pieces
    lookup = pltpu.make_async_copy(map_ref, table_ref, sems.at[pieces])
    lookup.start()
    copies = []
    for i in range(pieces):
        span = pl.ds(i * rows, rows)
        copies.append(pltpu.make_async_copy(source_ref.at[span], stage_ref.at[span], sems.at[i]))
        copies[i].start()
    lookup.wait()
    mine, theirs = spots(table_ref, sub_count)
    for i in range(pieces):
        copies[i].wait()
        span = pl.ds(i * rows, rows)
        for cycle in range(2):
            start = pl.multiple_of(mine[cycle] * block, block)
            mine_ref[span, pl.ds(cycle * block, block)] = stage_ref[span, pl.ds(start, block)]
    for cycle in range(2):
        start = pl.multiple_of(theirs[cycle] * block, block)
        lanes = pl.ds(cycle * block, block)
        head_ref[:, lanes] = stage_ref[pl.ds(0, head), pl.ds(start, block)]
        tail_ref[:, lanes] = stage_ref[pl.ds(head, depth - head), pl.ds(start, block)]


def local_kernel(
    tile,
    a_ref,
    mine_ref,
    head_ref,
    tail_ref,
    mass_ref,
    turned_ref,
    before_mine_ref,
    before_theirs_ref,
    columns_ref,
):
    depth, width = mine_ref.shape
    head = head_ref.shape[0]
    turned_ref[pl.ds(0, width), :] = mine_ref[...].T
    turned_ref[pl.ds(width, width), pl.ds(0, head)] = head_ref[...].T
    turned_ref[pl.ds(width, width), pl.ds(head, depth - head)] = tail_ref[...].T
    lanes = columns_ref.shape[1]
    for i in range(depth // lanes):
        line = mass_ref[:, pl.ds(i * lanes, lanes)]
        columns_ref[pl.ds(i * lanes, lanes), :] = jnp.broadcast_to(line, (lanes, lanes)).T
    near = pl.multiple_of(lax.axis_index("col") * depth, depth)
    for i in range(depth // tile):
        part = pl.ds(i * tile, tile)
        a = a_ref[part, pl.ds(near, depth)]
        before_mine_ref[part, :] = ndot(a, mine_ref[...])
        before_theirs_ref[part, :] = ndot(a[:, :head], head_ref[...]) + ndot(a[:, head:], tail_ref[...])


def middle_kernel(tile, a_ref, got_ref, before_ref, after_ref):
    depth = before_ref.shape[0]
    head = got_ref.shape[0]
    far = pl.multiple_of((1 - lax.axis_index("col")) * depth, depth)
    for i in range(depth // tile):
        part = pl.ds(i * tile, tile)
        after_ref[part, :] = before_ref[part, :] + ndot(a_ref[part, pl.ds(far, head)], got_ref[...])


def first_kernel(
    tile,
    sub_count,
    block,
    map_ref,
    a_ref,
    got_ref,
    before_ref,
    columns_ref,
    turned_ref,
    modes_ref,
    trial_high_ref,
    trial_low_ref,
    edge_ref,
    weight_ref,
    low_ref,
    high_ref,
    square_ref,
    turned_w_ref,
    small_ref,
    g_ref,
    w_ref,
):
    depth, width = got_ref.shape
    even = is_even()
    mine, theirs = spots(map_ref, sub_count)
    far = pl.ds(pl.multiple_of((1 - lax.axis_index("col")) * depth, depth), depth)
    for i in range(depth // tile):
        part = pl.ds(i * tile, tile)
        g = (-(before_ref[part, :] + ndot(a_ref[part, far], got_ref[...]))).astype(BF16)
        w = scaled(columns_ref[part, :], g)
        g_ref[part, :] = g
        w_ref[part, :] = w
    stiff = ndot(turned_ref[...], g_ref[...])
    of_mine = (stiff[:width] + edge_panel(mine, theirs, edge_ref, block)).astype(BF16)
    of_theirs = (stiff[width:] + edge_panel(theirs, theirs, edge_ref, block)).astype(BF16)
    low_ref[...] = jnp.where(even, of_theirs, of_mine)
    high_ref[...] = jnp.where(even, of_mine, of_theirs)
    turned_w_ref[...] = w_ref[...].T
    square = ndot(turned_w_ref[...], g_ref[...])
    square_ref[...] = (square + edge_diagonal(theirs, weight_ref, block)).astype(BF16)
    trial = jnp.where(even, trial_low_ref[...], trial_high_ref[...])
    upper, lower = halves(ndot(modes_ref[...], w_ref[...]))
    small_ref[...] = rdot(trial, upper) + rdot(trial, lower)


def second_kernel(
    tile,
    a_ref,
    got_ref,
    before_ref,
    columns_ref,
    turned_w_ref,
    square_ref,
    modes_ref,
    trial_high_ref,
    trial_low_ref,
    small_in_ref,
    mass_low_ref,
    mass_high_ref,
    g_ref,
    w_ref,
    crossed_ref,
    small_ref,
):
    depth, width = before_ref.shape
    tail = got_ref.shape[0]
    even = is_even()
    far = pl.multiple_of((1 - lax.axis_index("col")) * depth + depth - tail, tail)
    for i in range(depth // tile):
        part = pl.ds(i * tile, tile)
        g = (-(before_ref[part, :] + ndot(a_ref[part, pl.ds(far, tail)], got_ref[...]))).astype(BF16)
        g_ref[part, :] = g
        w_ref[part, :] = scaled(columns_ref[part, :], g)
    crossed = ndot(turned_w_ref[...], g_ref[...])
    crossed_ref[...] = crossed
    mixed = crossed.T.astype(BF16)
    square = square_ref[...]
    mass_low_ref[...] = jnp.where(even, square, mixed)
    mass_high_ref[pl.ds(0, width), :] = jnp.where(even, mixed, square)
    trial = jnp.where(even, trial_high_ref[...], trial_low_ref[...])
    upper, lower = halves(ndot(modes_ref[...], w_ref[...]))
    small = small_in_ref[...] + rdot(trial, upper) + rdot(trial, lower)
    small_ref[...] = small
    count, modes_count = small.shape
    mass_high_ref[pl.ds(width, count), :] = jnp.concatenate(
        [small, jnp.zeros((count, width - modes_count), F32)], axis=1
    ).astype(BF16)


def third_kernel(
    sub_count, block, map_ref, g_ref, w_ref, crossed_ref, turned_ref, edge_ref, weight_ref, back_ref, own_ref
):
    width = g_ref.shape[1]
    even = is_even()
    mine, theirs = spots(map_ref, sub_count)
    stiff = ndot(turned_ref[...], g_ref[...])
    of_mine = stiff[:width] + edge_panel(mine, mine, edge_ref, block)
    of_theirs = stiff[width:] + edge_panel(theirs, mine, edge_ref, block)
    inner = tdot(g_ref[...], w_ref[...]) + edge_diagonal(mine, weight_ref, block)
    crossed = crossed_ref[...]
    back_ref[0] = jnp.where(even, of_theirs, of_mine).astype(BF16)
    back_ref[1] = jnp.where(even, crossed, inner).astype(BF16)
    own_ref[0] = jnp.where(even, of_mine, of_theirs)
    own_ref[1] = jnp.where(even, inner, crossed)


def place_kernel(
    which,
    sub_count,
    block,
    own_ref,
    high_ref,
    back_ref,
    cross_ref,
    small_ref,
    out_ref,
    total_ref,
    kept_ref,
    moved_ref,
    stage_ref,
    sum_ref,
    sems,
):
    width = 2 * block
    copies = []
    if which == 1:
        count, modes_count = small_ref.shape
        other = high_ref[pl.ds(width, count), :].astype(F32)
        sum_ref[...] = small_ref[...] + other[:, :modes_count]
        copies.append(pltpu.make_async_copy(sum_ref, total_ref, sems.at[4]))
        copies[0].start()
    half = stage_ref.shape[2] // 2
    sub = lax.axis_index("sub")
    even = is_even()
    moved = back_ref[which].astype(F32) + cross_ref[...].astype(F32)
    kept = own_ref[which] + high_ref[pl.ds(0, width), :].astype(F32)
    kept = kept + jnp.where(even, moved, 0.0)
    moved = jnp.where(even, 0.0, moved)
    for k in range(2):
        kept_ref[k] = kept[:, k * block : (k + 1) * block]
        moved_ref[k] = moved[:, k * block : (k + 1) * block]
    kept_spot = lax.div(jnp.where(even, sub, lax.rem(sub + sub_count - 1, sub_count)), 2)
    moved_spot = lax.div(jnp.where(even, sub, lax.rem(sub + 1, sub_count)), 2)
    place = lax.broadcasted_iota(jnp.int32, (half, block), 0)
    kept_here = place == kept_spot
    moved_here = place == moved_spot
    group = 16
    chunks = 2
    rows = block // chunks
    for p in range(2):
        for chunk in range(chunks):

            def fill(step, carry, p=p, chunk=chunk):
                base = pl.multiple_of(step * group, group)
                for x in range(group):
                    row = chunk * rows + base + x
                    parts = []
                    for k in range(2):
                        source = pl.ds(p * block + row, 1)
                        a = jnp.broadcast_to(kept_ref[k, source, :], (half, block))
                        b = jnp.broadcast_to(moved_ref[k, source, :], (half, block))
                        parts.append(jnp.where(kept_here, a, jnp.where(moved_here, b, 0.0)))
                    stage_ref[p, row] = jnp.concatenate(parts, axis=0).astype(BF16)
                return carry

            lax.fori_loop(0, rows // group, fill, 0)
            span = pl.ds(chunk * rows, rows)
            copy = pltpu.make_async_copy(
                stage_ref.at[p, span], out_ref.at[p, span], sems.at[p * chunks + chunk]
            )
            copy.start()
            copies.append(copy)
    for copy in copies:
        copy.wait()


VM = pl.BlockSpec(memory_space=pltpu.VMEM)
SM = pl.BlockSpec(memory_space=pltpu.SMEM)
HB = pl.BlockSpec(memory_space=pltpu.HBM)


def place(own, high, back, cross, small, which, sub_count, block, cycles):
    width = 2 * block
    return pl.pallas_call(
        functools.partial(place_kernel, which, sub_count, block),
        in_specs=[VM, VM, VM, VM, VM],
        out_specs=[HB, HB],
        out_shape=[
            jax.ShapeDtypeStruct((2, block, cycles, block), BF16),
            jax.ShapeDtypeStruct(small.shape if which == 1 else (8, block), F32),
        ],
        scratch_shapes=[
            pltpu.VMEM((2, width, block), F32),
            pltpu.VMEM((2, width, block), F32),
            pltpu.VMEM((2, block, cycles, block), BF16),
            pltpu.VMEM(small.shape, F32),
            pltpu.SemaphoreType.DMA((5,)),
        ],
        compiler_params=pltpu.CompilerParams(vmem_limit_bytes=8 << 20),
        cost_estimate=cost(width * cycles * block * 8, 2 * width * cycles * block),
    )(own, in_vmem(high), in_vmem(back), in_vmem(cross), small)


def in_hbm(x):
    return pltpu.with_memory_space_constraint(x, pltpu.HBM)


def pick(sub_count, block, own_map, rows, tail):
    depth = rows.shape[0]
    width = 2 * block
    return pl.pallas_call(
        functools.partial(pick_kernel, sub_count, block),
        in_specs=[HB, HB],
        out_specs=[VM] * 3,
        out_shape=[
            pltpu.VMEM((depth, width), rows.dtype),
            pltpu.VMEM((depth - tail, width), rows.dtype),
            pltpu.VMEM((tail, width), rows.dtype),
        ],
        scratch_shapes=[
            pltpu.SMEM(own_map.shape, jnp.int32),
            pltpu.VMEM(rows.shape, rows.dtype),
            pltpu.SemaphoreType.DMA((3,)),
        ],
        compiler_params=pltpu.CompilerParams(vmem_limit_bytes=4 << 20),
        cost_estimate=cost(depth * block, 8 * depth * block),
        name="pick",
    )(in_hbm(own_map), in_hbm(rows))


def pair_shards(
    interior_inverse,
    interface_coupling,
    boundary_stiffness,
    interior_mass,
    boundary_mass,
    interior_modes,
    block_map,
    trial_vectors,
):
    depth = interior_inverse.shape[1]
    block = trial_vectors.shape[2]
    width = 2 * block
    trials = trial_vectors.shape[0]
    modes_count = interior_modes.shape[1]
    sub_count = lax.axis_size("sub")
    cycles = sub_count
    tile = depth // 3
    swap = [(0, 1), (1, 0)]
    both = ("sub", "col")
    back_route = [(i, (i - 1) % sub_count) for i in range(sub_count)]
    cross_route = [
        (2 * i + c, 2 * ((i - 1) % sub_count) + 1 - c) for i in range(sub_count) for c in range(2)
    ]
    params = pltpu.CompilerParams(vmem_limit_bytes=12 << 20)
    mine, head, tail = pick(sub_count, block, block_map, interface_coupling[0], depth // 4)
    got_theirs = in_vmem(lax.ppermute(mine, "col", swap))
    got_head = in_vmem(lax.ppermute(head, "col", swap))
    got_tail = in_vmem(lax.ppermute(tail, "col", swap))
    previous_trial = shifted(trial_vectors, "sub", 1)
    trial_high = in_vmem(trial_vectors.reshape(trials, width))
    trial_low = in_vmem(previous_trial.reshape(trials, width))
    inverse_rows = in_vmem(interior_inverse[0])
    edge = in_vmem(boundary_stiffness[0])
    modes = in_vmem(interior_modes[0])
    weights = in_vmem(boundary_mass[0].reshape(2, block))

    turned, before_mine, before_theirs, columns = pl.pallas_call(
        functools.partial(local_kernel, tile),
        in_specs=[VM] * 5,
        out_specs=[VM] * 4,
        out_shape=[
            pltpu.VMEM((2 * width, depth), BF16),
            pltpu.VMEM((depth, width), F32),
            pltpu.VMEM((depth, width), F32),
            pltpu.VMEM((depth, block), F32),
        ],
        compiler_params=params,
        cost_estimate=cost(4 * depth * depth * width, 2 * depth * depth),
        name="local",
    )(inverse_rows, mine, head, tail, in_vmem(interior_mass))
    stiff_low, stiff_high, square, turned_w, small_first = pl.pallas_call(
        functools.partial(first_kernel, tile, sub_count, block),
        in_specs=[SM] + [VM] * 10,
        out_specs=[VM] * 5,
        out_shape=[
            pltpu.VMEM((width, width), BF16),
            pltpu.VMEM((width, width), BF16),
            pltpu.VMEM((width, width), BF16),
            pltpu.VMEM((width, depth), BF16),
            pltpu.VMEM((trials, modes_count), F32),
        ],
        scratch_shapes=[pltpu.VMEM((depth, width), BF16), pltpu.VMEM((depth, width), BF16)],
        compiler_params=params,
        cost_estimate=cost(4 * depth * depth * width, 2 * depth * depth),
        name="first",
    )(
        block_map,
        inverse_rows,
        got_theirs,
        before_theirs,
        columns,
        turned,
        modes,
        trial_high,
        trial_low,
        edge,
        weights,
    )
    cross_stiff = lax.ppermute(stiff_low, both, cross_route)
    high_stiff = lax.ppermute(stiff_high, "col", swap)
    after_mine = pl.pallas_call(
        functools.partial(middle_kernel, tile),
        in_specs=[VM] * 3,
        out_specs=VM,
        out_shape=pltpu.VMEM((depth, width), F32),
        compiler_params=params,
        cost_estimate=cost(2 * depth * depth * width, 2 * depth * depth),
        name="middle",
    )(inverse_rows, got_head, before_mine)
    mass_low, mass_high, g_mine, w_mine, crossed, small = pl.pallas_call(
        functools.partial(second_kernel, tile),
        in_specs=[VM] * 10,
        out_specs=[VM] * 6,
        out_shape=[
            pltpu.VMEM((width, width), BF16),
            pltpu.VMEM((width + trials, width), BF16),
            pltpu.VMEM((depth, width), BF16),
            pltpu.VMEM((depth, width), BF16),
            pltpu.VMEM((width, width), F32),
            pltpu.VMEM((trials, modes_count), F32),
        ],
        compiler_params=params,
        cost_estimate=cost(2 * depth * depth * width, 2 * depth * depth),
        name="second",
    )(
        inverse_rows,
        got_tail,
        after_mine,
        columns,
        turned_w,
        square,
        modes,
        trial_high,
        trial_low,
        small_first,
    )
    back, own = pl.pallas_call(
        functools.partial(third_kernel, sub_count, block),
        in_specs=[SM] + [VM] * 6,
        out_specs=[VM] * 2,
        out_shape=[pltpu.VMEM((2, width, width), BF16), pltpu.VMEM((2, width, width), F32)],
        compiler_params=params,
        cost_estimate=cost(8 * depth * width * width, 10 * depth * width),
        name="third",
    )(block_map, g_mine, w_mine, crossed, turned, edge, weights)
    back_here = lax.ppermute(back, "sub", back_route)
    cross_mass = lax.ppermute(mass_low, both, cross_route)
    high_mass = lax.ppermute(mass_high, "col", swap)
    reduced_stiffness, _ = place(
        own, high_stiff, back_here, cross_stiff, small, 0, sub_count, block, cycles
    )
    reduced_mass, summed = place(
        own, high_mass, back_here, cross_mass, small, 1, sub_count, block, cycles
    )
    return (reduced_stiffness, reduced_mass, summed[None])


def solution(mesh):
    placed = (
        P("sub", "col", None),
        P("sub", "col", None),
        P("sub", "col", None),
        P("sub", "col"),
        P("sub", "col"),
        P("sub", None, "col"),
        P("sub", None),
        P(None, None, "sub"),
    )
    paired = mesh.shape["col"] == 2 and mesh.shape["sub"] % 2 == 0
    return jax.shard_map(
        pair_shards if paired else shards,
        mesh=mesh,
        in_specs=placed,
        out_specs=(P(None, "sub", None, "col"), P(None, "sub", None, "col"), P("sub", None, None)),
        check_vma=False,
    )
```

```python
import functools
import jax
import jax.numpy as jnp
from jax import lax
from jax.experimental import pallas as pl
from jax.experimental.pallas import tpu as pltpu
from jax.sharding import PartitionSpec as P


def shifted(block, axis, distance):
    devices = range(lax.axis_size(axis))
    route = [((i - distance) % len(devices), i) for i in devices]
    return lax.ppermute(block, axis, route)


def shards(
    interior_inverse,
    interface_coupling,
    boundary_stiffness,
    interior_mass,
    boundary_mass,
    interior_modes,
    block_map,
    trial_vectors,
):
    inverse_rows = interior_inverse[0]
    coupling_rows = interface_coupling[0]
    boundary_width = coupling_rows.shape[1]
    block_size = trial_vectors.shape[2]
    block_count = boundary_width // block_size
    sub_count = lax.axis_size("sub")
    grid_columns = lax.axis_size("col")
    sub_index = lax.axis_index("sub")
    column_index = lax.axis_index("col")
    previous_sub = (sub_index + sub_count - 1) % sub_count
    cycles = 2 * sub_count // grid_columns
    highest = lax.Precision.HIGHEST
    guyan_sum = jnp.dot(
        inverse_rows,
        lax.all_gather(coupling_rows, "col", axis=0, tiled=True),
        preferred_element_type=jnp.float32,
    )
    guyan = (-guyan_sum).astype(jnp.bfloat16)
    stiff_rows = boundary_stiffness[0]
    row_share = stiff_rows.shape[0]
    row_offset = column_index * row_share
    stiff_part = jnp.einsum("rb,rc->bc", coupling_rows, guyan, preferred_element_type=jnp.float32)
    stiff_part = lax.dynamic_update_slice_in_dim(
        stiff_part,
        lax.dynamic_slice_in_dim(stiff_part, row_offset, row_share, 0) + stiff_rows,
        row_offset,
        0,
    )
    weighted = (interior_mass[0][:, None] * guyan.astype(jnp.float32)).astype(jnp.bfloat16)
    mass_part = jnp.einsum("rb,rc->bc", guyan, weighted, preferred_element_type=jnp.float32)
    diagonal_rows = jnp.where(
        jnp.arange(boundary_width, dtype=jnp.int32)[None, :]
        == (row_offset + jnp.arange(row_share, dtype=jnp.int32))[:, None],
        boundary_mass[0][:, None],
        0.0,
    )
    mass_part = lax.dynamic_update_slice_in_dim(
        mass_part,
        lax.dynamic_slice_in_dim(mass_part, row_offset, row_share, 0) + diagonal_rows,
        row_offset,
        0,
    )
    previous_trial = shifted(trial_vectors, "sub", 1)
    candidates = jnp.concatenate([trial_vectors, previous_trial], axis=1)
    labels = jnp.stack([sub_index, sub_index + sub_count, previous_sub, previous_sub + sub_count])
    own_map = block_map[0]
    chooser = (own_map[:, None] == labels[None, :]).astype(jnp.bfloat16)
    local_trial = (
        jnp.einsum("tkb,ik->tib", candidates, chooser, preferred_element_type=jnp.float32)
        .astype(jnp.bfloat16)
        .reshape(trial_vectors.shape[0], boundary_width)
    )
    projected = jnp.einsum("rj,tj->tr", weighted, local_trial, preferred_element_type=jnp.float32)
    small_part = jnp.einsum(
        "tr,mr->tm", projected, interior_modes[0].astype(jnp.float32), precision=highest
    )
    stiffness, mass_sum, small_sum = lax.psum((stiff_part, mass_part, small_part), "col")
    stiff_blocks = stiffness.reshape(block_count, block_size, block_count, block_size)
    mass_blocks = mass_sum.reshape(block_count, block_size, block_count, block_size)
    row_cycles = jnp.arange(2, dtype=jnp.int32)

    def rows_for(owner_row):
        return (own_map[None, :] == row_cycles[:, None] * sub_count + owner_row).astype(jnp.float32)

    placement = (
        own_map[:, None]
        == jnp.arange(cycles, dtype=jnp.int32)[None, :] * grid_columns + column_index
    ).astype(jnp.float32)

    def select_rows(selection, blocks):
        return jnp.einsum("ri,ixjy->rxjy", selection, blocks, precision=highest)

    def spread(panel, where):
        return jnp.einsum("rxjy,jc->rxcy", panel, where, precision=highest)

    own_selection = rows_for(sub_index)
    own_stiff = spread(select_rows(own_selection, stiff_blocks), placement)
    own_mass = spread(select_rows(own_selection, mass_blocks), placement)
    leaving = rows_for(previous_sub)
    leaving_stiff = select_rows(leaving, stiff_blocks)
    leaving_mass = select_rows(leaving, mass_blocks)
    neighbour_stiff, neighbour_mass, neighbour_place = shifted(
        (leaving_stiff, leaving_mass, placement), "sub", -1
    )
    reduced_stiffness = (own_stiff + spread(neighbour_stiff, neighbour_place)).astype(jnp.bfloat16)
    reduced_mass = (own_mass + spread(neighbour_mass, neighbour_place)).astype(jnp.bfloat16)
    return (reduced_stiffness, reduced_mass, small_sum[None])


BF16, F32 = jnp.bfloat16, jnp.float32


def in_vmem(x):
    return pltpu.with_memory_space_constraint(x, pltpu.VMEM)


def cost(flops, moved):
    return pl.CostEstimate(flops=int(flops), bytes_accessed=int(moved), transcendentals=0)


def tdot(a, b):
    return lax.dot_general(a, b, (((0,), (0,)), ((), ())), preferred_element_type=F32)


def ndot(a, b):
    return jnp.dot(a, b, preferred_element_type=F32)


def rdot(a, b):
    return lax.dot_general(a, b, (((1,), (1,)), ((), ())), preferred_element_type=F32)


def is_even():
    return (lax.axis_index("sub") & 1) == lax.axis_index("col")


def spot(map_ref, parity, cycle, sub_count):
    found = jnp.int32(0)
    for i in range(4):
        label = map_ref[0, i]
        hit = ((label & 1) == parity) & ((label >= sub_count) == (cycle == 1))
        found += jnp.where(hit, i, 0)
    return found


def spots(map_ref, sub_count):
    column = lax.axis_index("col")
    return [
        [spot(map_ref, parity, cycle, sub_count) for cycle in range(2)]
        for parity in (column, 1 - column)
    ]


def edge_panel(row_places, column_places, edge_ref, block):
    column = lax.axis_index("col")
    rows = []
    for place in row_places:
        local = place - 2 * column
        inside = (local >= 0) & (local < 2)
        row = pl.multiple_of(jnp.clip(local, 0, 1) * block, block)
        cells = []
        for other in column_places:
            start = pl.multiple_of(other * block, block)
            cells.append(jnp.where(inside, edge_ref[pl.ds(row, block), pl.ds(start, block)], 0.0))
        rows.append(jnp.concatenate(cells, axis=1))
    return jnp.concatenate(rows, axis=0)


def edge_diagonal(places, weight_ref, block):
    column = lax.axis_index("col")
    width = 2 * block
    rows = lax.broadcasted_iota(jnp.int32, (width, width), 0)
    columns = lax.broadcasted_iota(jnp.int32, (width, width), 1)
    parts = []
    for place in places:
        local = place - 2 * column
        inside = (local >= 0) & (local < 2)
        parts.append(jnp.where(inside, weight_ref[pl.ds(jnp.clip(local, 0, 1), 1), :], 0.0))
    return jnp.where(rows == columns, jnp.concatenate(parts, axis=1), 0.0)


def scaled(mass, g):
    half = mass.shape[1]
    wide = g.astype(F32)
    return jnp.concatenate([wide[:, :half] * mass, wide[:, half:] * mass], axis=1).astype(BF16)


def halves(array):
    upper = array.astype(BF16)
    return upper, (array - upper.astype(F32)).astype(BF16)


def lead_kernel(sub_count, block, map_ref, source_ref, lead_ref, table_ref, stage_ref, sems):
    lookup = pltpu.make_async_copy(map_ref, table_ref, sems.at[0])
    lookup.start()
    copy = pltpu.make_async_copy(source_ref.at[pl.ds(0, lead_ref.shape[0])], stage_ref, sems.at[1])
    copy.start()
    lookup.wait()
    mine, _ = spots(table_ref, sub_count)
    copy.wait()
    for cycle in range(2):
        start = pl.multiple_of(mine[cycle] * block, block)
        lead_ref[:, pl.ds(cycle * block, block)] = stage_ref[:, pl.ds(start, block)]


def pick_kernel(
    sub_count, block, map_ref, source_ref, rest_ref, head_ref, tail_ref, table_ref, stage_ref, sems
):
    depth = source_ref.shape[0]
    head = head_ref.shape[0]
    lead = depth - rest_ref.shape[0]
    pieces = 2
    rows = depth // pieces
    lookup = pltpu.make_async_copy(map_ref, table_ref, sems.at[pieces])
    lookup.start()
    copies = []
    for i in range(pieces):
        span = pl.ds(i * rows, rows)
        copies.append(pltpu.make_async_copy(source_ref.at[span], stage_ref.at[span], sems.at[i]))
        copies[i].start()
    lookup.wait()
    mine, theirs = spots(table_ref, sub_count)
    for copy in copies:
        copy.wait()
    for cycle in range(2):
        start = pl.multiple_of(mine[cycle] * block, block)
        lanes = pl.ds(cycle * block, block)
        rest_ref[:, lanes] = stage_ref[pl.ds(lead, depth - lead), pl.ds(start, block)]
    for cycle in range(2):
        start = pl.multiple_of(theirs[cycle] * block, block)
        lanes = pl.ds(cycle * block, block)
        head_ref[:, lanes] = stage_ref[pl.ds(0, head), pl.ds(start, block)]
        tail_ref[:, lanes] = stage_ref[pl.ds(head, depth - head), pl.ds(start, block)]


def local_kernel(
    tile,
    a_ref,
    lead_ref,
    rest_ref,
    head_ref,
    tail_ref,
    mass_ref,
    turned_ref,
    before_mine_ref,
    before_theirs_ref,
    columns_ref,
):
    depth, width = before_mine_ref.shape
    lead = lead_ref.shape[0]
    head = head_ref.shape[0]
    turned_ref[pl.ds(0, width), pl.ds(0, lead)] = lead_ref[...].T
    turned_ref[pl.ds(0, width), pl.ds(lead, depth - lead)] = rest_ref[...].T
    turned_ref[pl.ds(width, width), pl.ds(0, head)] = head_ref[...].T
    turned_ref[pl.ds(width, width), pl.ds(head, depth - head)] = tail_ref[...].T
    lanes = columns_ref.shape[1]
    for i in range(depth // lanes):
        line = mass_ref[:, pl.ds(i * lanes, lanes)]
        columns_ref[pl.ds(i * lanes, lanes), :] = jnp.broadcast_to(line, (lanes, lanes)).T
    near = pl.multiple_of(lax.axis_index("col") * depth, depth)
    for i in range(depth // tile):
        part = pl.ds(i * tile, tile)
        a = a_ref[part, pl.ds(near, depth)]
        before_mine_ref[part, :] = ndot(a[:, :lead], lead_ref[...]) + ndot(a[:, lead:], rest_ref[...])
        before_theirs_ref[part, :] = ndot(a[:, :head], head_ref[...]) + ndot(a[:, head:], tail_ref[...])


def middle_kernel(tile, a_ref, got_ref, before_ref, after_ref):
    depth = before_ref.shape[0]
    head = got_ref.shape[0]
    far = pl.multiple_of((1 - lax.axis_index("col")) * depth, depth)
    for i in range(depth // tile):
        part = pl.ds(i * tile, tile)
        after_ref[part, :] = before_ref[part, :] + ndot(a_ref[part, pl.ds(far, head)], got_ref[...])


def first_kernel(
    tile,
    sub_count,
    block,
    map_ref,
    a_ref,
    lead_ref,
    rest_ref,
    before_ref,
    columns_ref,
    turned_ref,
    modes_ref,
    trial_high_ref,
    trial_low_ref,
    edge_ref,
    weight_ref,
    low_ref,
    high_ref,
    square_ref,
    turned_w_ref,
    small_ref,
    g_ref,
    w_ref,
):
    depth, width = before_ref.shape
    lead = lead_ref.shape[0]
    even = is_even()
    mine, theirs = spots(map_ref, sub_count)
    far = pl.multiple_of((1 - lax.axis_index("col")) * depth, depth)
    for i in range(depth // tile):
        part = pl.ds(i * tile, tile)
        a = a_ref[part, pl.ds(far, depth)]
        total = before_ref[part, :] + ndot(a[:, :lead], lead_ref[...]) + ndot(a[:, lead:], rest_ref[...])
        g = (-total).astype(BF16)
        w = scaled(columns_ref[part, :], g)
        g_ref[part, :] = g
        w_ref[part, :] = w
    stiff = ndot(turned_ref[...], g_ref[...])
    of_mine = (stiff[:width] + edge_panel(mine, theirs, edge_ref, block)).astype(BF16)
    of_theirs = (stiff[width:] + edge_panel(theirs, theirs, edge_ref, block)).astype(BF16)
    low_ref[...] = jnp.where(even, of_theirs, of_mine)
    high_ref[...] = jnp.where(even, of_mine, of_theirs)
    turned_w_ref[...] = w_ref[...].T
    square = ndot(turned_w_ref[...], g_ref[...])
    square_ref[...] = (square + edge_diagonal(theirs, weight_ref, block)).astype(BF16)
    trial = jnp.where(even, trial_low_ref[...], trial_high_ref[...])
    upper, lower = halves(ndot(modes_ref[...], w_ref[...]))
    small_ref[...] = rdot(trial, upper) + rdot(trial, lower)


def second_kernel(
    tile,
    a_ref,
    got_ref,
    before_ref,
    columns_ref,
    turned_w_ref,
    square_ref,
    modes_ref,
    trial_high_ref,
    trial_low_ref,
    small_in_ref,
    mass_low_ref,
    mass_high_ref,
    g_ref,
    w_ref,
    crossed_ref,
    small_ref,
):
    depth, width = before_ref.shape
    tail = got_ref.shape[0]
    even = is_even()
    far = pl.multiple_of((1 - lax.axis_index("col")) * depth + depth - tail, tail)
    for i in range(depth // tile):
        part = pl.ds(i * tile, tile)
        g = (-(before_ref[part, :] + ndot(a_ref[part, pl.ds(far, tail)], got_ref[...]))).astype(BF16)
        g_ref[part, :] = g
        w_ref[part, :] = scaled(columns_ref[part, :], g)
    crossed = ndot(turned_w_ref[...], g_ref[...])
    crossed_ref[...] = crossed
    mixed = crossed.T.astype(BF16)
    square = square_ref[...]
    mass_low_ref[...] = jnp.where(even, square, mixed)
    mass_high_ref[pl.ds(0, width), :] = jnp.where(even, mixed, square)
    trial = jnp.where(even, trial_high_ref[...], trial_low_ref[...])
    upper, lower = halves(ndot(modes_ref[...], w_ref[...]))
    small = small_in_ref[...] + rdot(trial, upper) + rdot(trial, lower)
    small_ref[...] = small
    count, modes_count = small.shape
    mass_high_ref[pl.ds(width, count), :] = jnp.concatenate(
        [small, jnp.zeros((count, width - modes_count), F32)], axis=1
    ).astype(BF16)


def third_kernel(
    sub_count, block, map_ref, g_ref, w_ref, crossed_ref, turned_ref, edge_ref, weight_ref, back_ref, own_ref
):
    width = g_ref.shape[1]
    even = is_even()
    mine, theirs = spots(map_ref, sub_count)
    stiff = ndot(turned_ref[...], g_ref[...])
    of_mine = stiff[:width] + edge_panel(mine, mine, edge_ref, block)
    of_theirs = stiff[width:] + edge_panel(theirs, mine, edge_ref, block)
    inner = tdot(g_ref[...], w_ref[...]) + edge_diagonal(mine, weight_ref, block)
    crossed = crossed_ref[...]
    back_ref[0] = jnp.where(even, of_theirs, of_mine).astype(BF16)
    back_ref[1] = jnp.where(even, crossed, inner).astype(BF16)
    own_ref[0] = jnp.where(even, of_mine, of_theirs)
    own_ref[1] = jnp.where(even, inner, crossed)


def place_kernel(
    which,
    sub_count,
    block,
    own_ref,
    high_ref,
    back_ref,
    cross_ref,
    small_ref,
    out_ref,
    total_ref,
    kept_ref,
    moved_ref,
    stage_ref,
    sum_ref,
    sems,
):
    width = 2 * block
    copies = []
    if which == 1:
        count, modes_count = small_ref.shape
        other = high_ref[pl.ds(width, count), :].astype(F32)
        sum_ref[...] = small_ref[...] + other[:, :modes_count]
        copies.append(pltpu.make_async_copy(sum_ref, total_ref, sems.at[4]))
        copies[0].start()
    half = stage_ref.shape[2] // 2
    sub = lax.axis_index("sub")
    even = is_even()
    moved = back_ref[which].astype(F32) + cross_ref[...].astype(F32)
    kept = own_ref[which] + high_ref[pl.ds(0, width), :].astype(F32)
    kept = kept + jnp.where(even, moved, 0.0)
    moved = jnp.where(even, 0.0, moved)
    for k in range(2):
        kept_ref[k] = kept[:, k * block : (k + 1) * block]
        moved_ref[k] = moved[:, k * block : (k + 1) * block]
    before = jnp.where(sub == 0, sub_count - 1, sub - 1)
    after = jnp.where(sub == sub_count - 1, 0, sub + 1)
    kept_spot = jnp.where(even, sub, before) >> 1
    moved_spot = jnp.where(even, sub, after) >> 1
    place = lax.broadcasted_iota(jnp.int32, (half, block), 0)
    kept_here = place == kept_spot
    moved_here = place == moved_spot
    group = 16
    chunks = 2
    rows = block // chunks
    for p in range(2):
        for chunk in range(chunks):

            def fill(step, carry, p=p, chunk=chunk):
                base = pl.multiple_of(step * group, group)
                for x in range(group):
                    row = chunk * rows + base + x
                    parts = []
                    for k in range(2):
                        source = pl.ds(p * block + row, 1)
                        a = jnp.broadcast_to(kept_ref[k, source, :], (half, block))
                        b = jnp.broadcast_to(moved_ref[k, source, :], (half, block))
                        parts.append(jnp.where(kept_here, a, jnp.where(moved_here, b, 0.0)))
                    stage_ref[p, row] = jnp.concatenate(parts, axis=0).astype(BF16)
                return carry

            lax.fori_loop(0, rows // group, fill, 0)
            span = pl.ds(chunk * rows, rows)
            copy = pltpu.make_async_copy(
                stage_ref.at[p, span], out_ref.at[p, span], sems.at[p * chunks + chunk]
            )
            copy.start()
            copies.append(copy)
    for copy in copies:
        copy.wait()


VM = pl.BlockSpec(memory_space=pltpu.VMEM)
SM = pl.BlockSpec(memory_space=pltpu.SMEM)
HB = pl.BlockSpec(memory_space=pltpu.HBM)


def place(own, high, back, cross, small, which, sub_count, block, cycles):
    width = 2 * block
    return pl.pallas_call(
        functools.partial(place_kernel, which, sub_count, block),
        in_specs=[VM, VM, VM, VM, VM],
        out_specs=[HB, HB],
        out_shape=[
            jax.ShapeDtypeStruct((2, block, cycles, block), BF16),
            jax.ShapeDtypeStruct(small.shape if which == 1 else (8, block), F32),
        ],
        scratch_shapes=[
            pltpu.VMEM((2, width, block), F32),
            pltpu.VMEM((2, width, block), F32),
            pltpu.VMEM((2, block, cycles, block), BF16),
            pltpu.VMEM(small.shape, F32),
            pltpu.SemaphoreType.DMA((5,)),
        ],
        compiler_params=pltpu.CompilerParams(vmem_limit_bytes=8 << 20),
        cost_estimate=cost(width * cycles * block * 8, 2 * width * cycles * block),
    )(own, in_vmem(high), in_vmem(back), in_vmem(cross), small)


def in_hbm(x):
    return pltpu.with_memory_space_constraint(x, pltpu.HBM)


def pick_lead(sub_count, block, own_map, rows, lead):
    width = 2 * block
    return pl.pallas_call(
        functools.partial(lead_kernel, sub_count, block),
        in_specs=[HB, HB],
        out_specs=VM,
        out_shape=pltpu.VMEM((lead, width), rows.dtype),
        scratch_shapes=[
            pltpu.SMEM(own_map.shape, jnp.int32),
            pltpu.VMEM((lead, rows.shape[1]), rows.dtype),
            pltpu.SemaphoreType.DMA((2,)),
        ],
        compiler_params=pltpu.CompilerParams(vmem_limit_bytes=2 << 20),
        cost_estimate=cost(lead * block, 8 * lead * block),
        name="lead",
    )(own_map, rows)


def pick(sub_count, block, own_map, rows, lead, tail):
    depth = rows.shape[0]
    width = 2 * block
    return pl.pallas_call(
        functools.partial(pick_kernel, sub_count, block),
        in_specs=[HB, HB],
        out_specs=[VM] * 3,
        out_shape=[
            pltpu.VMEM((depth - lead, width), rows.dtype),
            pltpu.VMEM((depth - tail, width), rows.dtype),
            pltpu.VMEM((tail, width), rows.dtype),
        ],
        scratch_shapes=[
            pltpu.SMEM(own_map.shape, jnp.int32),
            pltpu.VMEM(rows.shape, rows.dtype),
            pltpu.SemaphoreType.DMA((3,)),
        ],
        compiler_params=pltpu.CompilerParams(vmem_limit_bytes=4 << 20),
        cost_estimate=cost(depth * block, 8 * depth * block),
        name="pick",
    )(own_map, rows)


def pair_shards(
    interior_inverse,
    interface_coupling,
    boundary_stiffness,
    interior_mass,
    boundary_mass,
    interior_modes,
    block_map,
    trial_vectors,
):
    depth = interior_inverse.shape[1]
    block = trial_vectors.shape[2]
    width = 2 * block
    trials = trial_vectors.shape[0]
    modes_count = interior_modes.shape[1]
    sub_count = lax.axis_size("sub")
    cycles = sub_count
    tile = depth // 3
    swap = [(0, 1), (1, 0)]
    both = ("sub", "col")
    back_route = [(i, (i - 1) % sub_count) for i in range(sub_count)]
    cross_route = [
        (2 * i + c, 2 * ((i - 1) % sub_count) + 1 - c) for i in range(sub_count) for c in range(2)
    ]
    params = pltpu.CompilerParams(vmem_limit_bytes=12 << 20)
    own_map, coupling_rows = in_hbm(block_map), in_hbm(interface_coupling[0])
    lead = pick_lead(sub_count, block, own_map, coupling_rows, depth // 4)
    got_lead = in_vmem(lax.ppermute(lead, "col", swap))
    rest, head, tail = pick(sub_count, block, own_map, coupling_rows, depth // 4, depth // 12)
    got_rest = in_vmem(lax.ppermute(rest, "col", swap))
    got_head = in_vmem(lax.ppermute(head, "col", swap))
    got_tail = in_vmem(lax.ppermute(tail, "col", swap))
    previous_trial = shifted(trial_vectors, "sub", 1)
    trial_high = in_vmem(trial_vectors.reshape(trials, width))
    trial_low = in_vmem(previous_trial.reshape(trials, width))
    inverse_rows = in_vmem(interior_inverse[0])
    edge = in_vmem(boundary_stiffness[0])
    modes = in_vmem(interior_modes[0])
    weights = in_vmem(boundary_mass[0].reshape(2, block))

    turned, before_mine, before_theirs, columns = pl.pallas_call(
        functools.partial(local_kernel, tile),
        in_specs=[VM] * 6,
        out_specs=[VM] * 4,
        out_shape=[
            pltpu.VMEM((2 * width, depth), BF16),
            pltpu.VMEM((depth, width), F32),
            pltpu.VMEM((depth, width), F32),
            pltpu.VMEM((depth, block), F32),
        ],
        compiler_params=params,
        cost_estimate=cost(4 * depth * depth * width, 2 * depth * depth),
        name="local",
    )(inverse_rows, lead, rest, head, tail, in_vmem(interior_mass))
    stiff_low, stiff_high, square, turned_w, small_first = pl.pallas_call(
        functools.partial(first_kernel, tile, sub_count, block),
        in_specs=[SM] + [VM] * 11,
        out_specs=[VM] * 5,
        out_shape=[
            pltpu.VMEM((width, width), BF16),
            pltpu.VMEM((width, width), BF16),
            pltpu.VMEM((width, width), BF16),
            pltpu.VMEM((width, depth), BF16),
            pltpu.VMEM((trials, modes_count), F32),
        ],
        scratch_shapes=[pltpu.VMEM((depth, width), BF16), pltpu.VMEM((depth, width), BF16)],
        compiler_params=params,
        cost_estimate=cost(4 * depth * depth * width, 2 * depth * depth),
        name="first",
    )(
        block_map,
        inverse_rows,
        got_lead,
        got_rest,
        before_theirs,
        columns,
        turned,
        modes,
        trial_high,
        trial_low,
        edge,
        weights,
    )
    cross_stiff = lax.ppermute(stiff_low, both, cross_route)
    high_stiff = lax.ppermute(stiff_high, "col", swap)
    after_mine = pl.pallas_call(
        functools.partial(middle_kernel, tile),
        in_specs=[VM] * 3,
        out_specs=VM,
        out_shape=pltpu.VMEM((depth, width), F32),
        compiler_params=params,
        cost_estimate=cost(2 * depth * depth * width, 2 * depth * depth),
        name="middle",
    )(inverse_rows, got_head, before_mine)
    mass_low, mass_high, g_mine, w_mine, crossed, small = pl.pallas_call(
        functools.partial(second_kernel, tile),
        in_specs=[VM] * 10,
        out_specs=[VM] * 6,
        out_shape=[
            pltpu.VMEM((width, width), BF16),
            pltpu.VMEM((width + trials, width), BF16),
            pltpu.VMEM((depth, width), BF16),
            pltpu.VMEM((depth, width), BF16),
            pltpu.VMEM((width, width), F32),
            pltpu.VMEM((trials, modes_count), F32),
        ],
        compiler_params=params,
        cost_estimate=cost(2 * depth * depth * width, 2 * depth * depth),
        name="second",
    )(
        inverse_rows,
        got_tail,
        after_mine,
        columns,
        turned_w,
        square,
        modes,
        trial_high,
        trial_low,
        small_first,
    )
    back, own = pl.pallas_call(
        functools.partial(third_kernel, sub_count, block),
        in_specs=[SM] + [VM] * 6,
        out_specs=[VM] * 2,
        out_shape=[pltpu.VMEM((2, width, width), BF16), pltpu.VMEM((2, width, width), F32)],
        compiler_params=params,
        cost_estimate=cost(8 * depth * width * width, 10 * depth * width),
        name="third",
    )(block_map, g_mine, w_mine, crossed, turned, edge, weights)
    back_here = lax.ppermute(back, "sub", back_route)
    cross_mass = lax.ppermute(mass_low, both, cross_route)
    high_mass = lax.ppermute(mass_high, "col", swap)
    reduced_stiffness, _ = place(
        own, high_stiff, back_here, cross_stiff, small, 0, sub_count, block, cycles
    )
    reduced_mass, summed = place(
        own, high_mass, back_here, cross_mass, small, 1, sub_count, block, cycles
    )
    return (reduced_stiffness, reduced_mass, summed[None])


def solution(mesh):
    placed = (
        P("sub", "col", None),
        P("sub", "col", None),
        P("sub", "col", None),
        P("sub", "col"),
        P("sub", "col"),
        P("sub", None, "col"),
        P("sub", None),
        P(None, None, "sub"),
    )
    paired = mesh.shape["col"] == 2 and mesh.shape["sub"] % 2 == 0
    return jax.shard_map(
        pair_shards if paired else shards,
        mesh=mesh,
        in_specs=placed,
        out_specs=(P(None, "sub", None, "col"), P(None, "sub", None, "col"), P("sub", None, None)),
        check_vma=False,
    )
```
